8 devices in a mesh: rep: 2 (over y, z), dp: 4 (over x, core).
Axes of the slice: x: 2, y: 2, z: 1, core: 2. Of those that a mesh axis runs over, the one named last changes fastest.
Arguments:
- x: bfloat16 [8, 2048, 1280], P(('rep', 'dp')), parts along dimension 0
- dy: bfloat16 [8, 2048, 1280], P(('rep', 'dp')), parts along dimension 0
- w_gate: bfloat16 [2, 1280, 4096], P(None, 'dp')
- w_up: bfloat16 [2, 1280, 4096], P(None, 'dp')
- w_down: bfloat16 [2, 4096, 1280], P(None, 'dp')
Outputs:
- output 1: bfloat16 [8, 2048, 1280], P(('rep', 'dp')), parts along dimension 0
- output 2: bfloat16 [4, 1280, 4096], P('rep', 'dp'), parts along dimension 0
- output 3: bfloat16 [4, 1280, 4096], P('rep', 'dp'), parts along dimension 0
- output 4: bfloat16 [4, 4096, 1280], P('rep', 'dp'), parts along dimension 0
There are 2 independent parts. The reference program is written for one: setup_inputs(seed, part) draws one part's arguments, and reference() takes and returns one part's arrays. A program takes and returns all parts, laid end to end along the dimension named above; an argument that names none is the same for every part.
All inputs are finite; a program needn't handle non-finite values.
Results may differ from the reference program's by a relative error of at most 0.018.
Values are sent between devices in bfloat16 or wider.
A program may use at most 2 GiB of HBM per device.

```python
import jax
import jax.numpy as jnp
from jax import lax

SEQUENCES = 4
TOKENS = 2048
D = 1280
FF = 4096
LAYERS = 2
NAMES = ("w_gate", "w_up", "w_down")
SHAPES = {"w_gate": (LAYERS, D, FF), "w_up": (LAYERS, D, FF), "w_down": (LAYERS, FF, D)}


def bump(key, n, height):
    away = (jnp.arange(n, dtype=jnp.int32) - jax.random.randint(key, (), 0, n, jnp.int32)) % n
    return jnp.where(away < n // 8, height, 1.0)


def together(key, own, strength):
    shared = jax.random.normal(key, own.shape[1:], jnp.float32)
    return (own + strength * shared) * lax.rsqrt(1 + strength * strength)


def setup_inputs(seed: int = 0, part: int = 0) -> dict:
    kx, kdy, ka, kb, kz, kf, kh, kl, *kw = jax.random.split(jax.random.key(seed), 8 + len(NAMES))
    kx, kdy, ka, kb = (jax.random.fold_in(k, part) for k in (kx, kdy, ka, kb))
    shape = (SEQUENCES, TOKENS, D)
    much_x, much_dy = jax.random.uniform(kz, (2,), jnp.float32, 0.0, 1.0)
    layers = 2.0 ** jax.random.uniform(kl, (LAYERS, 1, 1), jnp.float32, -1.0, 1.0)
    x = together(ka, jax.random.normal(kx, shape, jnp.float32), much_x) * bump(kf, D, 4.0)
    dy = together(kb, jax.random.normal(kdy, shape, jnp.float32), much_dy)
    drawn = {"x": x.astype(jnp.bfloat16), "dy": (dy * (SEQUENCES * TOKENS) ** -0.5).astype(jnp.bfloat16)}
    for key, name in zip(kw, NAMES, strict=True):
        w = jax.random.normal(key, SHAPES[name], jnp.float32) * SHAPES[name][1] ** -0.5
        drawn[name] = (w * {"w_gate": 1.0, "w_up": bump(kh, FF, 4.0), "w_down": layers}[name]).astype(jnp.bfloat16)
    return drawn


def matmul(a, w):
    return jnp.dot(a, w, preferred_element_type=jnp.float32).astype(jnp.bfloat16)


def normed(h):
    wide = h.astype(jnp.float32)
    scale = lax.rsqrt(jnp.mean(wide**2, -1, keepdims=True) + 1e-6)
    return (wide * scale).astype(jnp.bfloat16)


def layer(h, w):
    a = normed(h)
    gate = jnp.dot(a, w["w_gate"], preferred_element_type=jnp.float32)
    up = jnp.dot(a, w["w_up"], preferred_element_type=jnp.float32)
    return h + matmul((jax.nn.silu(gate) * up).astype(jnp.bfloat16), w["w_down"])


def stack(weights, h):
    return lax.scan(lambda h, w: (layer(h, w), None), h, weights)[0]


def reference(x, dy, w_gate, w_up, w_down):
    weights = dict(zip(NAMES, (w_gate, w_up, w_down), strict=True))

    def take(so_far, sequence):
        h, by_y = sequence
        _, back = jax.vjp(stack, weights, h)
        by_weights, by_h = back(by_y)
        return jax.tree.map(lambda total, term: total + term.astype(jnp.float32), so_far, by_weights), by_h

    none_yet = {name: jnp.zeros(w.shape, jnp.float32) for name, w in weights.items()}
    by_weights, by_x = lax.scan(take, none_yet, (x, dy))
    return (by_x, *(by_weights[name].astype(jnp.bfloat16) for name in NAMES))
```

```python
import jax
import jax.numpy as jnp
from jax import lax
from jax.experimental import pallas as pl
from jax.experimental.pallas import tpu as pltpu
from jax.sharding import PartitionSpec as P

F32, BF16 = jnp.float32, jnp.bfloat16
AXES = ("rep", "dp")
TOKENS, D, FF, LAYERS = 2048, 1280, 4096, 2
DB, FB = D // 4, FF // 4
NN, NT = (((1,), (0,)), ((), ())), (((1,), (1,)), ((), ()))
MESH = pl.DeviceIdType.MESH
TM, TN = 512, 512


def dot(a, b, dims=NN):
    return lax.dot_general(a, b, dims, preferred_element_type=F32)


def pipe(body, grid, ins, outs, *refs):
    def step(at, *blocks):
        body(at.index, *blocks)

    pltpu.emit_pipeline(step, grid=grid, in_specs=ins, out_specs=outs, _explicit_indices=True)(*refs)


def place():
    r, d = lax.axis_index("rep"), lax.axis_index("dp")
    return r, d, d // 2, d % 2


def greet(devices):
    barrier = pltpu.get_barrier_semaphore()
    for device in devices:
        pl.semaphore_signal(barrier, inc=1, device_id=device, device_id_type=MESH)
    pl.semaphore_wait(barrier, len(devices))


def inverse(wide):
    return lax.rsqrt(jnp.mean(wide * wide, -1, keepdims=True) + 1e-6)


STRIPS = 4
CHUNKS = []
for _l in range(LAYERS):
    CHUNKS += [(_l, m, s) for s in range(STRIPS) for m in (0, 1)] + [(_l, 2, s) for s in range(STRIPS)]


def forward_kernel(x, dy, wg, wu, wd, fg, fu, fd, dy_t, a0_t, gate0, up0, mid0, h1, a1_t, gate1, up1, mid1, a, acc, own_send, own_recv, send, recv):
    r, d, chip, core = place()
    across, beside = (1 - chip) * 2 + core, chip * 2 + 1 - core
    over_x, over_y, over_chip = (r, across), (1 - r, d), (r, beside)
    shards, fulls = (wg, wu, wd), (fg, fu, fd)

    def region(chunk, block, half):
        l, m, s = chunk
        if m < 2:
            return l, pl.ds(pl.multiple_of(block * DB + half * (DB // 2), 32), DB // 2), pl.ds(s * (FF // STRIPS), FF // STRIPS)
        rows = FB // 2 // STRIPS
        return l, pl.ds(pl.multiple_of(block * FB + half * (FB // 2) + s * rows, 32), rows), slice(None)

    def copy(kind, k, src, dst, device):
        return pltpu.make_async_remote_copy(src, dst, send.at[kind, k], recv.at[kind, k], device_id=device, device_id_type=MESH)

    def x_copy(k):
        m = CHUNKS[k][1]
        return copy(0, k, shards[m].at[region(CHUNKS[k], 0, r)], fulls[m].at[region(CHUNKS[k], d, r)], over_x)

    def passed(kind, k, half, device):
        part = fulls[CHUNKS[k][1]].at[region(CHUNKS[k], across, half)]
        return copy(kind, k, part, part, device)

    def y_copy(k):
        return passed(1, k, r, over_y)

    def first_copy(k):
        return passed(2, k, r, over_chip)

    def second_copy(k):
        return passed(3, k, 1 - r, over_chip)

    def own_copy(l, m):
        rows = shards[m].shape[1]
        to = fulls[m].at[l, pl.ds(pl.multiple_of(d * rows, 32), rows)]
        return pltpu.make_async_remote_copy(shards[m].at[l], to, own_send.at[l * 3 + m], own_recv.at[l * 3 + m], device_id=over_chip, device_id_type=MESH)

    greet([over_x, over_y, over_chip])
    n = len(CHUNKS)
    for k in range(n):
        x_copy(k).start()
    for l in range(LAYERS):
        for m in range(3):
            own_copy(l, m).start()

    def event(k):
        if k < n:
            x_copy(k).wait_recv()
            y_copy(k).start()
            first_copy(k).start()
        if k:
            y_copy(k - 1).wait_recv()
            second_copy(k - 1).start()

    happened = [0]

    def upto(k):
        while happened[0] <= k:
            event(happened[0])
            happened[0] += 1

    def ready(ks):
        upto(max(ks) + 1)
        for k in ks:
            first_copy(k).wait_recv()
            second_copy(k).wait_recv()

    def at_steps(index, steps):
        for step in steps:
            @pl.when(index == step)
            def _(k=happened[0]):
                event(k)
            happened[0] += 1

    def move(_, src, dst):
        dst[...] = src[...]

    for m, rows in ((0, 160), (1, 160), (2, 512)):
        wide = shards[m].shape[2]
        pipe(move, (LAYERS, 2), [pl.BlockSpec((1, rows, wide), lambda l, i: (l, i, 0))],
             [pl.BlockSpec((1, rows, wide), lambda l, i: (l, d * 2 + i, 0))], shards[m], fulls[m])

    def prepare(at, x_ref, dy_ref, at_ref, dyt_ref):
        wide = x_ref[...].astype(F32)
        new = (wide * inverse(wide)).astype(BF16)
        a[pl.ds(at[0] * 256, 256), :] = new
        at_ref[...] = new.T
        dyt_ref[...] = dy_ref[...].T

    row, column = pl.BlockSpec((256, D), lambda i: (i, 0)), pl.BlockSpec((D, 256), lambda i: (0, i))
    pipe(prepare, (TOKENS // 256,), [row, row], [column, column], x, dy, a0_t, dy_t)

    def ffn(l, gate, up, mid, base, steps):
        for s in range(STRIPS):
            ready([base + 2 * s, base + 2 * s + 1])
            if s == 0:
                for m in (0, 1):
                    own_copy(l, m).wait_recv()
            cuts = FF // STRIPS // TN

            def body(at, wg_ref, wu_ref, gate_ref, up_ref, mid_ref):
                f, i = at
                at_steps(f * (TOKENS // TM) + i, steps)
                left = a[pl.ds(i * TM, TM), :]
                gate_ref[...] = dot(left, wg_ref[...])
                up_ref[...] = dot(left, wu_ref[...])
                g = gate_ref[...]
                mid_ref[...] = (jax.nn.sigmoid(g) * g * up_ref[...]).astype(BF16)

            before = happened[0]
            weight = pl.BlockSpec((D, TN), lambda f, i: (0, s * cuts + f))
            out = pl.BlockSpec((TM, TN), lambda f, i: (i, s * cuts + f))
            steps_now = steps

            def once(at, *refs, before=before):
                happened[0] = before
                body(at, *refs)

            pipe(once, (cuts, TOKENS // TM), [weight, weight], [out, out, out], fg.at[l], fu.at[l], gate, up, mid)
            happened[0] = before + len(steps_now)

    ffn(0, gate0, up0, mid0, 0, (4,))

    ready(list(range(8, 12)))
    own_copy(0, 2).wait_recv()
    before = happened[0]

    def down(at, mid_ref, w_ref):
        k, i = at
        happened[0] = before
        at_steps(k * (TOKENS // TM) + i, (3, 8, 13))
        rows = pl.ds(i * TM, TM)
        part = dot(mid_ref[...], w_ref[...])

        @pl.when(k == 0)
        def _():
            acc[rows, :] = part

        @pl.when(k > 0)
        def _():
            acc[rows, :] += part

    pipe(down, (4, TOKENS // TM), [pl.BlockSpec((TM, FF // 4), lambda k, i: (i, k)), pl.BlockSpec((FF // 4, D), lambda k, i: (k, 0))], [],
         mid0, fd.at[0])
    happened[0] = before + 3

    def next_state(at, x_ref, h_ref, at_ref):
        rows = pl.ds(at[0] * 256, 256)
        h = (x_ref[...].astype(F32) + acc[rows, :].astype(BF16).astype(F32)).astype(BF16)
        h_ref[...] = h
        wide = h.astype(F32)
        new = (wide * inverse(wide)).astype(BF16)
        a[rows, :] = new
        at_ref[...] = new.T

    pipe(next_state, (TOKENS // 256,), [row], [row, column], x, h1, a1_t)
    ffn(1, gate1, up1, mid1, 12, (0, 4))
    ready(list(range(20, 24)))
    own_copy(1, 2).wait_recv()
    for k in range(n):
        for c in (x_copy(k), y_copy(k), first_copy(k), second_copy(k)):
            c.wait_send()
    for l in range(LAYERS):
        for m in range(3):
            own_copy(l, m).wait_send()


UNITS = [(l, m, half) for l in (1, 0) for m in (2, 0, 1) for half in (0, 1)]
ROWS = ((2, DB, FF // 2), (2, DB, FF // 2), (2, D // 2, FB))


def backward_kernel(fg, fu, fd, dy, dy_t, x, h1, a0_t, a1_t, gate0, up0, mid0, gate1, up1, mid1,
                    dx, og, ou, od, dgate, dup, dh_t, theirs_g, mine_g, got_g, leaves_g, came_g, theirs_d, mine_d, got_d, leaves_d, came_d,
                    dh, acc, chip_send, chip_recv, x_send, x_recv):
    r, d, chip, core = place()
    over_x, over_chip = (r, (1 - chip) * 2 + core), (r, chip * 2 + 1 - core)
    grads, gates, ups, mids, a_t, d_t, states = (og, ou, od), (gate0, gate1), (up0, up1), (mid0, mid1), (a0_t, a1_t), (dh_t, dy_t), (x, h1)
    slots = {}
    for l, m, half in UNITS:
        kind = m == 2
        slots[l, m, half] = sum(1 for key in slots if (key[1] == 2) == kind)

    def buffers(u):
        at = slots[UNITS[u]]
        group = (theirs_d, mine_d, got_d, leaves_d, came_d) if UNITS[u][1] == 2 else (theirs_g, mine_g, got_g, leaves_g, came_g)
        return [ref.at[at] for ref in group]

    def chip_copy(u):
        theirs, _, got, _, _ = buffers(u)
        return pltpu.make_async_remote_copy(theirs, got, chip_send.at[u], chip_recv.at[u], device_id=over_chip, device_id_type=MESH)

    def x_copy(u):
        _, _, _, leaves, came = buffers(u)
        return pltpu.make_async_remote_copy(leaves, came, x_send.at[u], x_recv.at[u], device_id=over_x, device_id_type=MESH)

    def term(u):
        l, m, half = UNITS[u]
        theirs, mine, *_ = buffers(u)
        if m == 2:
            def body(at, left, to_send, to_keep, theirs_ref, mine_ref):
                theirs_ref[0] = dot(left[...], to_send[...]).astype(BF16)
                mine_ref[0] = dot(left[...], to_keep[...]).astype(BF16)

            cuts = FB // TN
            out = pl.BlockSpec((1, D // 2, TN), lambda j, t: (j, 0, t))
            pipe(body, (2, cuts), [
                pl.BlockSpec((D // 2, TOKENS), lambda j, t: (half, 0)),
                pl.BlockSpec((TOKENS, TN), lambda j, t: (0, (j * 2 + 1 - core) * cuts + t)),
                pl.BlockSpec((TOKENS, TN), lambda j, t: (0, (j * 2 + core) * cuts + t)),
            ], [out, out], d_t[l], mids[l], mids[l], theirs, mine)
        else:
            def body(at, left, right, theirs_ref, mine_ref):
                for j in range(2):
                    for ref, who in ((theirs_ref, 1 - core), (mine_ref, core)):
                        rows = pl.ds(pl.multiple_of((j * 2 + who) * DB, 64), DB)
                        ref[j] = dot(left[rows, :], right[...]).astype(BF16)

            cuts = FF // 2 // TN
            out = pl.BlockSpec((2, DB, TN), lambda t: (0, 0, t))
            pipe(body, (cuts,), [pl.BlockSpec((D, TOKENS), lambda t: (0, 0)), pl.BlockSpec((TOKENS, TN), lambda t: (0, half * cuts + t))],
                 [out, out], a_t[l], (dgate, dup)[m], theirs, mine)
        chip_copy(u).start()

    def leave(u):
        chip_copy(u).wait_recv()
        _, mine, got, leaves, _ = buffers(u)
        rows, wide = ROWS[UNITS[u][1]][1] // 2, ROWS[UNITS[u][1]][2]

        def body(at, mine_ref, got_ref, out_ref):
            out_ref[...] = (mine_ref[0].astype(F32) + got_ref[0].astype(F32)).astype(BF16)

        two = pl.BlockSpec((1, rows, wide), lambda i: (1 - chip, i, 0))
        pipe(body, (2,), [two, two], [pl.BlockSpec((rows, wide), lambda i: (i, 0))], mine, got, leaves)
        x_copy(u).start()

    def finish(u):
        x_copy(u).wait_recv()
        l, m, half = UNITS[u]
        _, mine, got, _, came = buffers(u)

        def body(at, mine_ref, got_ref, came_ref, out_ref):
            total = mine_ref[0].astype(F32) + got_ref[0].astype(F32) + came_ref[...].astype(F32)
            out_ref[...] = (total.T if m == 2 else total).astype(BF16)

        if m == 2:
            two = pl.BlockSpec((1, D // 2, 256), lambda i: (chip, 0, i))
            pipe(body, (FB // 256,), [two, two, pl.BlockSpec((D // 2, 256), lambda i: (0, i))], [pl.BlockSpec((256, D // 2), lambda i: (i, half))],
                 mine, got, came, grads[m].at[l])
        else:
            two = pl.BlockSpec((1, DB // 2, FF // 2), lambda i: (chip, i, 0))
            pipe(body, (2,), [two, two, pl.BlockSpec((DB // 2, FF // 2), lambda i: (i, 0))], [pl.BlockSpec((DB // 2, FF // 2), lambda i: (i, half))],
                 mine, got, came, grads[m].at[l])

    def by_mid(l, part):
        cuts = FF // TN // 2

        def body(at, w_ref, gate_ref, up_ref, dgate_ref, dup_ref):
            f, i = at
            by = dot(dh[pl.ds(i * TM, TM), :], w_ref[...], NT).astype(BF16).astype(F32)
            g = gate_ref[...]
            sig = jax.nn.sigmoid(g)
            dup_ref[...] = (by * (g * sig)).astype(BF16)
            dgate_ref[...] = (by * up_ref[...] * (sig * (1 + g * (1 - sig)))).astype(BF16)

        tile = pl.BlockSpec((TM, TN), lambda f, i: (i, part * cuts + f))
        pipe(body, (cuts, TOKENS // TM), [pl.BlockSpec((TN, D), lambda f, i: (part * cuts + f, 0)), tile, tile], [tile, tile],
             fd.at[l], gates[l], ups[l], dgate, dup)

    def by_a(l):
        def body(at, dg_ref, du_ref, wg_ref, wu_ref):
            k, i = at
            rows = pl.ds(i * TM, TM)
            part = dot(dg_ref[...], wg_ref[...], NT) + dot(du_ref[...], wu_ref[...], NT)

            @pl.when(k == 0)
            def _():
                acc[rows, :] = part

            @pl.when(k > 0)
            def _():
                acc[rows, :] += part

        left = pl.BlockSpec((TM, FF // 4), lambda k, i: (i, k))
        right = pl.BlockSpec((D, FF // 4), lambda k, i: (0, k))
        pipe(body, (4, TOKENS // TM), [left, left, right, right], [], dgate, dup, fg.at[l], fu.at[l])

    def by_h(l):
        def body(at, h_ref, out_ref):
            rows = pl.ds(at[0] * 256, 256)
            wide, da = h_ref[...].astype(F32), acc[rows, :]
            scale = inverse(wide)
            along = jnp.mean(da * wide, -1, keepdims=True)
            new = (dh[rows, :].astype(F32) + scale * (da - wide * (scale * scale * along))).astype(BF16)
            if l:
                dh[rows, :] = new
                out_ref[...] = new.T
            else:
                out_ref[...] = new

        row, column = pl.BlockSpec((256, D), lambda i: (i, 0)), pl.BlockSpec((D, 256), lambda i: (0, i))
        pipe(body, (TOKENS // 256,), [row], [column if l else row], states[l], dh_t if l else dx)

    greet([over_x, over_chip])
    pltpu.sync_copy(dy, dh)
    for l in (1, 0):
        u = 0 if l else 6
        if l == 0:
            by_mid(0, 0)
            by_mid(0, 1)
        term(u)
        term(u + 1)
        leave(u)
        if l:
            by_mid(1, 0)
        leave(u + 1)
        if l:
            by_mid(1, 1)
        term(u + 2)
        for v in range(u + 3, u + 6):
            term(v)
            leave(v - 1)
        by_a(l)
        leave(u + 5)
        by_h(l)
    for u in range(len(UNITS)):
        finish(u)
    for u in range(len(UNITS)):
        chip_copy(u).wait_send()
        x_copy(u).wait_send()


def shape(*dims, dtype=BF16):
    return jax.ShapeDtypeStruct(dims, dtype)


def call(kernel, outs, scratch, collective_id, flops, *args):
    anywhere = pl.BlockSpec(memory_space=pl.ANY)
    return pl.pallas_call(
        kernel, out_shape=outs, in_specs=[anywhere] * len(args), out_specs=[anywhere] * len(outs), scratch_shapes=scratch,
        compiler_params=pltpu.CompilerParams(collective_id=collective_id, has_side_effects=True, vmem_limit_bytes=60 * 2**20),
        cost_estimate=pl.CostEstimate(flops=flops, bytes_accessed=400_000_000, transcendentals=0),
    )(*args)


def body(x, dy, w_gate, w_up, w_down):
    x, dy = x[0], dy[0]
    matmul = 2 * TOKENS * D * FF
    hidden = [shape(TOKENS, FF, dtype=F32), shape(TOKENS, FF, dtype=F32), shape(TOKENS, FF)]
    dma = pltpu.SemaphoreType.DMA
    n = len(CHUNKS)
    fg, fu, fd, dy_t, a0_t, gate0, up0, mid0, h1, a1_t, gate1, up1, mid1 = call(
        forward_kernel,
        [shape(LAYERS, D, FF), shape(LAYERS, D, FF), shape(LAYERS, FF, D), shape(D, TOKENS), shape(D, TOKENS), *hidden, shape(TOKENS, D), shape(D, TOKENS), *hidden],
        [pltpu.VMEM((TOKENS, D), BF16), pltpu.VMEM((TOKENS, D), F32), dma((6,)), dma((6,)), dma((4, n)), dma((4, n))],
        0, 5 * matmul, x, dy, w_gate, w_up, w_down)
    two_g, two_d = shape(8, 2, DB, FF // 2), shape(4, 2, D // 2, FB)
    one_g, one_d = shape(8, DB, FF // 2), shape(4, D // 2, FB)
    units = len(UNITS)
    dx, og, ou, od, *_ = call(
        backward_kernel,
        [shape(TOKENS, D), shape(LAYERS, DB, FF), shape(LAYERS, DB, FF), shape(LAYERS, FB, D), shape(TOKENS, FF), shape(TOKENS, FF), shape(D, TOKENS),
         two_g, two_g, two_g, one_g, one_g, two_d, two_d, two_d, one_d, one_d],
        [pltpu.VMEM((TOKENS, D), BF16), pltpu.VMEM((TOKENS, D), F32)] + [dma((units,))] * 4,
        1, 12 * matmul, fg, fu, fd, dy, dy_t, x, h1, a0_t, a1_t, gate0, up0, mid0, gate1, up1, mid1)
    return dx[None], og, ou, od


def solution(mesh):
    own, rows = P(AXES), P(None, "dp")
    return jax.shard_map(body, mesh=mesh, in_specs=(own, own, rows, rows, rows), out_specs=(own, *[P("rep", "dp")] * 3), check_vma=False)
```

```python
import jax
import jax.numpy as jnp
from jax import lax
from jax.experimental import pallas as pl
from jax.experimental.pallas import tpu as pltpu
from jax.sharding import PartitionSpec as P

F32, BF16 = jnp.float32, jnp.bfloat16
AXES = ("rep", "dp")
TOKENS, D, FF, LAYERS = 2048, 1280, 4096, 2
DB, FB = D // 4, FF // 4
NN, NT = (((1,), (0,)), ((), ())), (((1,), (1,)), ((), ()))
MESH = pl.DeviceIdType.MESH
TM, TN = 1024, 512


def dot(a, b, dims=NN):
    return lax.dot_general(a, b, dims, preferred_element_type=F32)


def pipe(body, grid, ins, outs, *refs):
    def step(at, *blocks):
        body(at.index, *blocks)

    pltpu.emit_pipeline(step, grid=grid, in_specs=ins, out_specs=outs, trace_scopes=False, _explicit_indices=True)(*refs)


def place():
    r, d = lax.axis_index("rep"), lax.axis_index("dp")
    return r, d, d // 2, d % 2


def named(name, f, *args):
    with jax.named_scope(name):
        return f(*args)


def greet(devices):
    barrier = pltpu.get_barrier_semaphore()
    for device in devices:
        pl.semaphore_signal(barrier, inc=1, device_id=device, device_id_type=MESH)
    pl.semaphore_wait(barrier, len(devices))


def inverse(wide):
    return lax.rsqrt(jnp.mean(wide * wide, -1, keepdims=True) + 1e-6)


STRIPS = 4
WIDE = FF // STRIPS
CHUNKS = [(0, m, s) for s in range(STRIPS) for m in (0, 1)] + [(l, 2, s) for l in (0, 1) for s in range(STRIPS)]
CHUNKS += [(1, m, s) for s in range(STRIPS) for m in (0, 1)]


def kernel(x, dy, wg, wu, wd,
           fg, fu, fd, a0_t, a1_t, silu0, slope0, mids, h1, dgu, dx,
           out_g, got_g, leaves_g, came_g, stay_g, kept_g, out_d, got_d, leaves_d, came_d, stay_d, kept_d,
           a, dh, left_a, left_d, own_send, own_recv, send, recv, w_sem, chip_send, chip_recv, x_send, x_recv):
    r, d, chip, core = place()
    across, beside = (1 - chip) * 2 + core, chip * 2 + 1 - core
    over_x, over_y, over_chip = (r, across), (1 - r, d), (r, beside)
    shards, fulls = (wg, wu, wd), (fg, fu, fd)


    def region(chunk, block, half, first):
        l, m, s = chunk
        if m < 2:
            column = pl.multiple_of(((first * 2 + s) % 4) * WIDE, WIDE)
            return l, pl.ds(pl.multiple_of(block * DB + half * (DB // 2), 32), DB // 2), pl.ds(column, WIDE)
        rows = FB // 2 // STRIPS
        return l, pl.ds(pl.multiple_of(block * FB + half * (FB // 2) + s * rows, 32), rows), slice(None)

    def copy(kind, k, src, dst, device):
        return pltpu.make_async_remote_copy(src, dst, send.at[kind, k], recv.at[kind, k], device_id=device, device_id_type=MESH)

    def x_copy(k):
        m = CHUNKS[k][1]
        return copy(0, k, shards[m].at[region(CHUNKS[k], 0, r, chip)], fulls[m].at[region(CHUNKS[k], d, r, chip)], over_x)

    def passed(kind, k, half, device):
        part = fulls[CHUNKS[k][1]].at[region(CHUNKS[k], across, half, 1 - chip)]
        return copy(kind, k, part, part, device)

    def y_copy(k):
        return passed(1, k, r, over_y)

    def first_copy(k):
        return passed(2, k, r, over_chip)

    def second_copy(k):
        return passed(3, k, 1 - r, over_chip)

    def own_copy(l, m):
        rows = shards[m].shape[1]
        to = fulls[m].at[l, pl.ds(pl.multiple_of(d * rows, 32), rows)]
        return pltpu.make_async_remote_copy(shards[m].at[l], to, own_send.at[l * 3 + m], own_recv.at[l * 3 + m], device_id=over_chip, device_id_type=MESH)

    greet([over_x, over_y, over_chip])
    n = len(CHUNKS)
    for k in range(n):
        x_copy(k).start()
    for l in range(LAYERS):
        for m in range(3):
            own_copy(l, m).start()

    def pass_on(k):
        x_copy(k).wait_recv()
        y_copy(k).start()
        first_copy(k).start()

    def share(k):
        y_copy(k).wait_recv()
        second_copy(k).start()

    LAG = 2
    passed_on, shared = [0], [0]

    def due():
        k, first = passed_on[0], shared[0]
        passed_on[0] += 1
        shared[0] = max(first, passed_on[0] - LAG)
        return k, range(first, shared[0])

    def event(k, ks):
        pass_on(k)
        for other in ks:
            share(other)

    def upto(k):
        while passed_on[0] <= k:
            event(*due())

    def ready(ks):
        upto(max(ks))
        while shared[0] <= max(ks):
            share(shared[0])
            shared[0] += 1
        for k in ks:
            first_copy(k).wait_recv()
            second_copy(k).wait_recv()

    def eventful(name, body, grid, steps, *rest):
        plan = [(step, due()) for step in steps]

        def once(at, *refs):
            now = at[0] if len(grid) == 1 else at[0] * grid[1] + at[1]
            for step, what in plan:
                @pl.when(now == step)
                def _():
                    event(*what)
            body(at, *refs)

        named(name, pipe, once, grid, *rest)

    def move(_, src, dst):
        dst[...] = src[...]

    def place_own(l, m):
        rows, wide = shards[m].shape[1] // 2, shards[m].shape[2]
        named(f"move_{l}_{m}", pipe, move, (2,), [pl.BlockSpec((rows, wide), lambda i: (i, 0))], [pl.BlockSpec((rows, wide), lambda i: (d * 2 + i, 0))],
              shards[m].at[l], fulls[m].at[l])

    def prepare(at, x_ref, dy_ref, at_ref):
        rows = pl.ds(at[0] * 256, 256)
        wide = x_ref[...].astype(F32)
        new = (wide * inverse(wide)).astype(BF16)
        a[rows, :] = new
        at_ref[...] = new.T
        dh[rows, :] = dy_ref[...]
        left_d[:, rows] = dy_ref[...].T

    row, column = pl.BlockSpec((256, D), lambda i: (i, 0)), pl.BlockSpec((D, 256), lambda i: (0, i))
    named("prepare", pipe, prepare, (TOKENS // 256,), [row, row], [column], x, dy, a0_t)
    upto(0)
    place_own(0, 0)
    upto(1)
    place_own(0, 1)
    upto(2)

    def up_front(at, wg_ref, wu_ref, silu_ref, slope_ref, mid_ref):
        left = a[pl.ds(at[1] * TM, TM), :]
        g, u = dot(left, wg_ref[...]), dot(left, wu_ref[...])
        sig = jax.nn.sigmoid(g)
        silu = g * sig
        silu_ref[...] = silu
        slope_ref[...] = u * (sig + silu * (1 - sig))
        mid_ref[...] = (silu * u).astype(BF16)

    def last(at, wg_ref, wu_ref, wd_ref, mid_ref, dgate_ref, dup_ref):
        rows = pl.ds(at[1] * TM, TM)
        left = a[rows, :]
        g, u = dot(left, wg_ref[...]), dot(left, wu_ref[...])
        by = dot(dh[rows, :], wd_ref[...], NT).astype(BF16).astype(F32)
        sig = jax.nn.sigmoid(g)
        silu = g * sig
        mid_ref[...] = (silu * u).astype(BF16)
        dup_ref[...] = (by * silu).astype(BF16)
        dgate_ref[...] = (by * (u * (sig + silu * (1 - sig)))).astype(BF16)

    cuts = WIDE // TN

    def ffn(l, s, base, steps):
        named(f"ready_{l}_{s}", ready, [base + 2 * s, base + 2 * s + 1])
        if s == 0:
            for m in (0, 1):
                own_copy(l, m).wait_recv()
        at = ((1 - chip) * 2 + s) % 4 * cuts
        weight = pl.BlockSpec((D, TN), lambda f, i: (0, at + f))
        out = pl.BlockSpec((TM, TN), lambda f, i: (i, at + f))
        if l:
            eventful(f"ffn_{l}_{s}", last, (cuts, TOKENS // TM), steps, [weight, weight, pl.BlockSpec((TN, D), lambda f, i: (at + f, 0))],
                     [out, out, out], fg.at[l], fu.at[l], fd.at[l], mids.at[l], dgu.at[l, 0], dgu.at[l, 1])
        else:
            eventful(f"ffn_{l}_{s}", up_front, (cuts, TOKENS // TM), steps, [weight, weight], [out, out, out],
                     fg.at[l], fu.at[l], silu0, slope0, mids.at[l])

    for s, steps in enumerate(((1, 3), (0, 2), (0, 2), (0, 1, 3))):
        ffn(0, s, 0, steps)

    def down(w):
        pltpu.sync_copy(fd.at[0], w)

        def body(at, mid_ref, x_ref, h_ref, at_ref):
            rows = pl.ds(at[0] * 256, 256)
            h = (x_ref[...].astype(F32) + dot(mid_ref[...], w[...]).astype(BF16).astype(F32)).astype(BF16)
            h_ref[...] = h
            wide = h.astype(F32)
            new = (wide * inverse(wide)).astype(BF16)
            a[rows, :] = new
            left_a[:, rows] = new.T
            at_ref[...] = new.T

        eventful("down", body, (TOKENS // 256,), (2, 4, 6, 7), [pl.BlockSpec((256, FF), lambda i: (i, 0)), row], [row, column], mids.at[0], x, h1, a1_t)

    place_own(0, 2)
    upto(12)
    place_own(1, 0)
    place_own(1, 1)
    named("ready_down", ready, list(range(8, 12)))
    own_copy(0, 2).wait_recv()
    upto(13)
    pl.run_scoped(down, pltpu.VMEM((FF, D), BF16))
    place_own(1, 2)


    def buffers(l, m, leaving):
        if m == 2:
            return [ref.at[l] for ref in ((out_d, got_d) if leaving else (stay_d, kept_d))]
        return [ref.at[l, m] for ref in ((out_g, got_g) if leaving else (stay_g, kept_g))]

    def chip_copy(l, m, leaving):
        term, got = buffers(l, m, leaving)
        k = (l * 3 + m) * 2 + leaving
        return pltpu.make_async_remote_copy(term.at[1 - core], got, chip_send.at[k], chip_recv.at[k], device_id=over_chip, device_id_type=MESH)

    def over(l, m):
        return (leaves_d.at[l], came_d.at[l]) if m == 2 else (leaves_g.at[l, m], came_g.at[l, m])

    def cross(l, m):
        k = l * 3 + m
        return pltpu.make_async_remote_copy(*over(l, m), x_send.at[k], x_recv.at[k], device_id=over_x, device_id_type=MESH)

    def term_down(l, leaving):
        side = 1 - chip if leaving else chip
        to = buffers(l, 2, leaving)[0]

        def body(at, right, out_ref):
            out_ref[...] = dot(left_d[...], right[...]).astype(BF16)

        cuts = FB // TN
        if leaving:
            for first, who in ((True, 1 - core), (False, core)):
                block = (side * 2 + who) * cuts
                pipe(body, (cuts,), [pl.BlockSpec((TOKENS, TN), lambda t: (0, block + t))], [pl.BlockSpec((D, TN), lambda t: (0, t))], mids.at[l], to.at[who])
                if first:
                    chip_copy(l, 2, leaving).start()
        else:
            def both(at, right, out_ref):
                body(at, right, out_ref.at[0])

            pipe(both, (2, cuts), [pl.BlockSpec((TOKENS, TN), lambda w, t: (0, (side * 2 + w) * cuts + t))], [pl.BlockSpec((1, D, TN), lambda w, t: (w, 0, t))],
                 mids.at[l], to)
            chip_copy(l, 2, leaving).start()

    def term(l, leaving, ms):
        side = 1 - chip if leaving else chip
        to = (out_g if leaving else stay_g).at[l]
        base = ms[0]

        def body(at, right, out_ref):
            rows = pl.ds(pl.multiple_of(side * (2 * DB), 128), 2 * DB)
            both = dot(left_a[rows, :], right[0]).astype(BF16)
            out_ref[0, 0] = both[:DB]
            out_ref[0, 1] = both[DB:]

        pipe(body, (len(ms), FF // TN), [pl.BlockSpec((1, TOKENS, TN), lambda m, t: (base + m, 0, t))],
             [pl.BlockSpec((1, 2, DB, TN), lambda m, t: (base + m, 0, 0, t))], dgu.at[l], to)
        for m in ms:
            chip_copy(l, m, leaving).start()

    def leave(l, m):
        named("chip_wait", chip_copy(l, m, 1).wait_recv)
        term, got = buffers(l, m, 1)

        def body(at, mine_ref, got_ref, out_ref):
            out_ref[...] = (mine_ref[...].astype(F32) + got_ref[...].astype(F32)).astype(BF16)

        spec = pl.BlockSpec((D // 4, FB) if m == 2 else (DB // 4, FF), lambda i: (i, 0))
        pipe(body, (4,), [spec, spec], [spec], term.at[core], got, over(l, m)[0])
        cross(l, m).start()

    def leave_pair(l):
        for m in (0, 1):
            chip_copy(l, m, 1).wait_recv()

        def body(at, mine_ref, got_ref, out_ref):
            out_ref[0] = (mine_ref[0, 0].astype(F32) + got_ref[0].astype(F32)).astype(BF16)

        spec = pl.BlockSpec((1, DB // 4, FF), lambda m, i: (m, i, 0))
        pipe(body, (2, 4), [pl.BlockSpec((1, 1, DB // 4, FF), lambda m, i: (m, core, i, 0)), spec], [spec], out_g.at[l], got_g.at[l], leaves_g.at[l])
        for m in (0, 1):
            cross(l, m).start()

    def by_mid(l):
        rows = 1024

        def body(at, w_ref, silu_ref, slope_ref, dgate_ref, dup_ref):
            for c in range(rows // 256):
                part = slice(c * 256, c * 256 + 256)
                by = dot(dh[pl.ds(at[1] * rows + c * 256, 256), :], w_ref[...], NT).astype(BF16).astype(F32)
                dup_ref[part, :] = (by * silu_ref[part, :]).astype(BF16)
                dgate_ref[part, :] = (by * slope_ref[part, :]).astype(BF16)

        tile = pl.BlockSpec((rows, TN), lambda f, i: (i, f))
        pipe(body, (FF // TN, TOKENS // rows), [pl.BlockSpec((TN, D), lambda f, i: (f, 0)), tile, tile], [tile, tile],
             fd.at[l], silu0, slope0, dgu.at[l, 0], dgu.at[l, 1])

    def by_a(l, meanwhile):
        def scoped(g_w, u_w):
            copies = [pltpu.make_async_copy(full.at[l], w, w_sem.at[k]) for k, (full, w) in enumerate(((fg, g_w), (fu, u_w)))]
            for c in copies:
                c.start()
            meanwhile()
            for c in copies:
                c.wait()

            def body(at, dg_ref, du_ref, h_ref, *out_ref):
                rows = pl.ds(at[0] * 256, 256)
                da = dot(dg_ref[...], g_w[...], NT) + dot(du_ref[...], u_w[...], NT)
                wide = h_ref[...].astype(F32)
                scale = inverse(wide)
                along = jnp.mean(da * wide, -1, keepdims=True)
                new = (dh[rows, :].astype(F32) + scale * (da - wide * (scale * scale * along))).astype(BF16)
                if l:
                    dh[rows, :] = new
                    left_d[:, rows] = new.T
                else:
                    out_ref[0][...] = new

            tile = pl.BlockSpec((256, FF), lambda i: (i, 0))
            named(f"by_a_{l}", pipe, body, (TOKENS // 256,), [tile, tile, row], [] if l else [row], dgu.at[l, 0], dgu.at[l, 1], h1 if l else x, *([] if l else [dx]))

        pl.run_scoped(scoped, pltpu.VMEM((D, FF), BF16), pltpu.VMEM((D, FF), BF16))

    def do(what, *args):
        named("_".join([what.__name__, *[str(v).replace(" ", "") for v in args]]), what, *args)

    named("ready_last", ready, list(range(12, 16)))
    own_copy(1, 2).wait_recv()
    ffn(1, 0, 16, (0, 0, 2, 3))
    ffn(1, 1, 16, (1, 2))
    do(term_down, 1, 1)
    do(leave, 1, 2)
    ffn(1, 2, 16, ())
    ffn(1, 3, 16, ())
    do(term, 1, 1, (0,))
    do(term, 1, 1, (1,))
    do(leave, 1, 0)
    do(leave, 1, 1)
    reload = pltpu.make_async_copy(a0_t, left_a, w_sem.at[2])
    reload.start()
    by_a(1, lambda: do(term_down, 1, 0))
    do(term_down, 0, 1)
    do(leave, 0, 2)
    do(by_mid, 0)
    reload.wait()
    do(term, 0, 1, (0, 1))
    do(term_down, 0, 0)
    do(leave_pair, 0)
    do(term, 0, 0, (0, 1))
    pltpu.sync_copy(a1_t, left_a)
    by_a(0, lambda: do(term, 1, 0, (0, 1)))
    with jax.named_scope("end"):
        for k in range(n):
            for c in (x_copy(k), y_copy(k), first_copy(k), second_copy(k)):
                c.wait_send()
        for l in range(LAYERS):
            for m in range(3):
                own_copy(l, m).wait_send()
                for leaving in (0, 1):
                    chip_copy(l, m, leaving).wait_send()
                chip_copy(l, m, 0).wait_recv()
                cross(l, m).wait()


def total(a, b, c):
    return a.astype(F32) + b.astype(F32) + c.astype(F32)


def finish_kernel(core, stay_g, kept_g, came_g, stay_u, kept_u, came_u, stay_d, kept_d, came_d, dx, og, ou, od, dx_out):
    og[0] = total(stay_g[0, 0, 0], kept_g[0, 0], came_g[0, 0]).astype(BF16)
    ou[0] = total(stay_u[0, 0, 0], kept_u[0, 0], came_u[0, 0]).astype(BF16)
    od[0] = total(stay_d[0, 0], kept_d[0], came_d[0]).astype(BF16).T
    dx_out[...] = dx[...]


def shape(*dims, dtype=BF16):
    return jax.ShapeDtypeStruct(dims, dtype)


def finish(core, stay_g, kept_g, came_g, stay_d, kept_d, came_d, dx):
    steps = 4
    rows, columns, tokens = DB // steps, FB // steps, TOKENS // (LAYERS * steps)
    ins = []
    for m in (0, 1):
        one = pl.BlockSpec((1, 1, rows, FF), lambda l, i, core, m=m: (l, m, i, 0))
        ins += [pl.BlockSpec((1, 1, 1, rows, FF), lambda l, i, core, m=m: (l, m, core[0], i, 0)), one, one]
    one = pl.BlockSpec((1, D, columns), lambda l, i, core: (l, 0, i))
    ins += [pl.BlockSpec((1, 1, D, columns), lambda l, i, core: (l, core[0], 0, i)), one, one]
    some = pl.BlockSpec((tokens, D), lambda l, i, core: (l * steps + i, 0))
    out = pl.BlockSpec((1, rows, FF), lambda l, i, core: (l, i, 0))
    return pl.pallas_call(
        finish_kernel, out_shape=[shape(LAYERS, DB, FF), shape(LAYERS, DB, FF), shape(LAYERS, FB, D), shape(TOKENS, D)],
        compiler_params=pltpu.CompilerParams(vmem_limit_bytes=60 * 2**20),
        grid_spec=pltpu.PrefetchScalarGridSpec(
            num_scalar_prefetch=1, grid=(LAYERS, steps), in_specs=[*ins, some],
            out_specs=[out, out, pl.BlockSpec((1, columns, D), lambda l, i, core: (l, i, 0)), some]),
    )(core, stay_g, kept_g, came_g, stay_g, kept_g, came_g, stay_d, kept_d, came_d, dx)


def body(x, dy, w_gate, w_up, w_down):
    x, dy = x[0], dy[0]
    dma, vmem = pltpu.SemaphoreType.DMA, pltpu.VMEM
    hidden, two_g, one_g, two_d, one_d = shape(LAYERS, TOKENS, FF), shape(LAYERS, 2, 2, DB, FF), shape(LAYERS, 2, DB, FF), shape(LAYERS, 2, D, FB), shape(LAYERS, D, FB)
    outs = dict(
        fg=shape(LAYERS, D, FF), fu=shape(LAYERS, D, FF), fd=shape(LAYERS, FF, D), a0_t=shape(D, TOKENS), a1_t=shape(D, TOKENS),
        silu0=shape(TOKENS, FF, dtype=F32), slope0=shape(TOKENS, FF, dtype=F32), mids=hidden, h1=shape(TOKENS, D), dgu=shape(LAYERS, 2, TOKENS, FF), dx=shape(TOKENS, D),
        out_g=two_g, got_g=one_g, leaves_g=one_g, came_g=one_g, stay_g=two_g, kept_g=one_g,
        out_d=two_d, got_d=one_d, leaves_d=one_d, came_d=one_d, stay_d=two_d, kept_d=one_d)
    n = len(CHUNKS)
    anywhere = pl.BlockSpec(memory_space=pl.ANY)
    done = pl.pallas_call(
        kernel, out_shape=list(outs.values()), in_specs=[anywhere] * 5, out_specs=[anywhere] * len(outs),
        scratch_shapes=[vmem((TOKENS, D), BF16), vmem((TOKENS, D), BF16), vmem((D, TOKENS), BF16), vmem((D, TOKENS), BF16), dma((6,)), dma((6,)), dma((4, n)), dma((4, n)),
                        dma((3,)), dma((12,)), dma((12,)), dma((6,)), dma((6,))],
        compiler_params=pltpu.CompilerParams(collective_id=0, has_side_effects=True, vmem_limit_bytes=60 * 2**20),
        cost_estimate=pl.CostEstimate(flops=17 * 2 * TOKENS * D * FF, bytes_accessed=800_000_000, transcendentals=0),
    )(x, dy, w_gate, w_up, w_down)
    done = dict(zip(outs, done))
    core = (lax.axis_index("dp") % 2).reshape(1).astype(jnp.int32)
    og, ou, od, dx = finish(core, *(done[k] for k in ("stay_g", "kept_g", "came_g", "stay_d", "kept_d", "came_d", "dx")))
    return dx[None], og, ou, od


def solution(mesh):
    own, rows = P(AXES), P(None, "dp")
    return jax.shard_map(body, mesh=mesh, in_specs=(own, own, rows, rows, rows), out_specs=(own, *[P("rep", "dp")] * 3), check_vma=False)
```

```python
import jax
import jax.numpy as jnp
from jax import lax
from jax.experimental import pallas as pl
from jax.experimental.pallas import tpu as pltpu
from jax.sharding import PartitionSpec as P

F32, BF16 = jnp.float32, jnp.bfloat16
AXES = ("rep", "dp")
TOKENS, D, FF, LAYERS = 2048, 1280, 4096, 2
DB, FB = D // 4, FF // 4
NN, NT = (((1,), (0,)), ((), ())), (((1,), (1,)), ((), ()))
MESH = pl.DeviceIdType.MESH
TM, TN = 1024, 512


def dot(a, b, dims=NN):
    return lax.dot_general(a, b, dims, preferred_element_type=F32)


def pipe(body, grid, ins, outs, *refs):
    def step(at, *blocks):
        body(at.index, *blocks)

    pltpu.emit_pipeline(step, grid=grid, in_specs=ins, out_specs=outs, trace_scopes=False, _explicit_indices=True)(*refs)


def place():
    r, d = lax.axis_index("rep"), lax.axis_index("dp")
    return r, d, d // 2, d % 2


def named(name, f, *args):
    with jax.named_scope(name):
        return f(*args)


def greet(devices):
    barrier = pltpu.get_barrier_semaphore()
    for device in devices:
        pl.semaphore_signal(barrier, inc=1, device_id=device, device_id_type=MESH)
    pl.semaphore_wait(barrier, len(devices))


def inverse(wide):
    return lax.rsqrt(jnp.mean(wide * wide, -1, keepdims=True) + 1e-6)


STRIPS = 4
WIDE = FF // STRIPS
CHUNKS = [(0, m, s) for s in range(STRIPS) for m in (0, 1)] + [(l, 2, s) for l in (0, 1) for s in range(STRIPS)]
CHUNKS += [(1, m, s) for s in range(STRIPS) for m in (0, 1)]


def kernel(x, dy, wg, wu, wd,
           fg, fu, fd, a0_t, a1_t, silu0, slope0, mids, h1, dgu, dx,
           out_g, got_g, leaves_g, came_g, stay_g, kept_g, out_d, got_d, leaves_d, came_d, stay_d, kept_d,
           a, dh, left_a, left_d, own_send, own_recv, send, recv, w_sem, chip_send, chip_recv, x_send, x_recv):
    r, d, chip, core = place()
    across, beside = (1 - chip) * 2 + core, chip * 2 + 1 - core
    over_x, over_y, over_chip = (r, across), (1 - r, d), (r, beside)
    shards, fulls = (wg, wu, wd), (fg, fu, fd)


    def region(chunk, block, half, first):
        l, m, s = chunk
        if m < 2:
            column = pl.multiple_of(((first * 2 + s) % 4) * WIDE, WIDE)
            return l, pl.ds(pl.multiple_of(block * DB + half * (DB // 2), 32), DB // 2), pl.ds(column, WIDE)
        rows = FB // 2 // STRIPS
        return l, pl.ds(pl.multiple_of(block * FB + half * (FB // 2) + s * rows, 32), rows), slice(None)

    def copy(kind, k, src, dst, device):
        return pltpu.make_async_remote_copy(src, dst, send.at[kind, k], recv.at[kind, k], device_id=device, device_id_type=MESH)

    def x_copy(k):
        m = CHUNKS[k][1]
        return copy(0, k, shards[m].at[region(CHUNKS[k], 0, r, chip)], fulls[m].at[region(CHUNKS[k], d, r, chip)], over_x)

    def passed(kind, k, half, device):
        part = fulls[CHUNKS[k][1]].at[region(CHUNKS[k], across, half, 1 - chip)]
        return copy(kind, k, part, part, device)

    def y_copy(k):
        return passed(1, k, r, over_y)

    def first_copy(k):
        return passed(2, k, r, over_chip)

    def second_copy(k):
        return passed(3, k, 1 - r, over_chip)

    def own_copy(l, m):
        rows = shards[m].shape[1]
        to = fulls[m].at[l, pl.ds(pl.multiple_of(d * rows, 32), rows)]
        return pltpu.make_async_remote_copy(shards[m].at[l], to, own_send.at[l * 3 + m], own_recv.at[l * 3 + m], device_id=over_chip, device_id_type=MESH)

    greet([over_x, over_y, over_chip])
    n = len(CHUNKS)
    for k in range(n):
        x_copy(k).start()
    for l in range(LAYERS):
        for m in range(3):
            own_copy(l, m).start()

    def pass_on(k):
        x_copy(k).wait_recv()
        y_copy(k).start()
        first_copy(k).start()

    def share(k):
        y_copy(k).wait_recv()
        second_copy(k).start()

    LAG = 2
    passed_on, shared = [0], [0]

    def due():
        k, first = passed_on[0], shared[0]
        passed_on[0] += 1
        shared[0] = max(first, passed_on[0] - LAG)
        return k, range(first, shared[0])

    def event(k, ks):
        pass_on(k)
        for other in ks:
            share(other)

    def upto(k):
        while passed_on[0] <= k:
            event(*due())

    def ready(ks):
        upto(max(ks))
        while shared[0] <= max(ks):
            share(shared[0])
            shared[0] += 1
        for k in ks:
            first_copy(k).wait_recv()
            second_copy(k).wait_recv()

    def eventful(name, body, grid, steps, *rest):
        plan = [(step, due()) for step in steps]

        def once(at, *refs):
            now = at[0] if len(grid) == 1 else at[0] * grid[1] + at[1]
            for step, what in plan:
                @pl.when(now == step)
                def _():
                    event(*what)
            body(at, *refs)

        named(name, pipe, once, grid, *rest)

    def move(_, src, dst):
        dst[...] = src[...]

    def place_own(l, m):
        rows, wide = shards[m].shape[1] // 2, shards[m].shape[2]
        named(f"move_{l}_{m}", pipe, move, (2,), [pl.BlockSpec((rows, wide), lambda i: (i, 0))], [pl.BlockSpec((rows, wide), lambda i: (d * 2 + i, 0))],
              shards[m].at[l], fulls[m].at[l])

    def prepare(at, x_ref, dy_ref, at_ref):
        rows = pl.ds(at[0] * 256, 256)
        wide = x_ref[...].astype(F32)
        new = (wide * inverse(wide)).astype(BF16)
        a[rows, :] = new
        at_ref[...] = new.T
        dh[rows, :] = dy_ref[...]
        left_d[:, rows] = dy_ref[...].T

    row, column = pl.BlockSpec((256, D), lambda i: (i, 0)), pl.BlockSpec((D, 256), lambda i: (0, i))
    place_own(0, 0)
    place_own(0, 1)
    eventful("prepare", prepare, (TOKENS // 256,), (1, 7), [row, row], [column], x, dy, a0_t)
    place_own(0, 2)
    upto(2)
    place_own(1, 0)

    def up_front(at, wg_ref, wu_ref, silu_ref, slope_ref, mid_ref):
        left = a[pl.ds(at[1] * TM, TM), :]
        g, u = dot(left, wg_ref[...]), dot(left, wu_ref[...])
        sig = jax.nn.sigmoid(g)
        silu = g * sig
        silu_ref[...] = silu
        slope_ref[...] = u * (sig + silu * (1 - sig))
        mid_ref[...] = (silu * u).astype(BF16)

    def last(at, wg_ref, wu_ref, wd_ref, mid_ref, dgate_ref, dup_ref):
        rows = pl.ds(at[1] * TM, TM)
        left = a[rows, :]
        g, u = dot(left, wg_ref[...]), dot(left, wu_ref[...])
        by = dot(dh[rows, :], wd_ref[...], NT).astype(BF16).astype(F32)
        sig = jax.nn.sigmoid(g)
        silu = g * sig
        mid_ref[...] = (silu * u).astype(BF16)
        dup_ref[...] = (by * silu).astype(BF16)
        dgate_ref[...] = (by * (u * (sig + silu * (1 - sig)))).astype(BF16)

    cuts = WIDE // TN

    def ffn(l, s, base, steps):
        named(f"ready_{l}_{s}", ready, [base + 2 * s, base + 2 * s + 1])
        if s == 0:
            for m in (0, 1):
                own_copy(l, m).wait_recv()
        at = ((1 - chip) * 2 + s) % 4 * cuts
        weight = pl.BlockSpec((D, TN), lambda f, i: (0, at + f))
        out = pl.BlockSpec((TM, TN), lambda f, i: (i, at + f))
        if l:
            eventful(f"ffn_{l}_{s}", last, (cuts, TOKENS // TM), steps, [weight, weight, pl.BlockSpec((TN, D), lambda f, i: (at + f, 0))],
                     [out, out, out], fg.at[l], fu.at[l], fd.at[l], mids.at[l], dgu.at[l, 0], dgu.at[l, 1])
        else:
            eventful(f"ffn_{l}_{s}", up_front, (cuts, TOKENS // TM), steps, [weight, weight], [out, out, out],
                     fg.at[l], fu.at[l], silu0, slope0, mids.at[l])

    for s, steps in enumerate(((1, 3), (0, 2), (0, 2), (0, 1, 2))):
        ffn(0, s, 0, steps)

    def down(w):
        pltpu.sync_copy(fd.at[0], w)

        def body(at, mid_ref, x_ref, h_ref, at_ref):
            rows = pl.ds(at[0] * 256, 256)
            h = (x_ref[...].astype(F32) + dot(mid_ref[...], w[...]).astype(BF16).astype(F32)).astype(BF16)
            h_ref[...] = h
            wide = h.astype(F32)
            new = (wide * inverse(wide)).astype(BF16)
            a[rows, :] = new
            left_a[:, rows] = new.T
            at_ref[...] = new.T

        eventful("down", body, (TOKENS // 256,), (0, 2, 4, 6), [pl.BlockSpec((256, FF), lambda i: (i, 0)), row], [row, column], mids.at[0], x, h1, a1_t)

    upto(12)
    place_own(1, 1)
    named("ready_down", ready, list(range(8, 12)))
    own_copy(0, 2).wait_recv()
    upto(13)
    pl.run_scoped(down, pltpu.VMEM((FF, D), BF16))
    place_own(1, 2)


    def buffers(l, m, leaving):
        if m == 2:
            return [ref.at[l] for ref in ((out_d, got_d) if leaving else (stay_d, kept_d))]
        return [ref.at[l, m] for ref in ((out_g, got_g) if leaving else (stay_g, kept_g))]

    def chip_copy(l, m, leaving):
        term, got = buffers(l, m, leaving)
        k = (l * 3 + m) * 2 + leaving
        return pltpu.make_async_remote_copy(term.at[1 - core], got, chip_send.at[k], chip_recv.at[k], device_id=over_chip, device_id_type=MESH)

    def over(l, m):
        return (leaves_d.at[l], came_d.at[l]) if m == 2 else (leaves_g.at[l, m], came_g.at[l, m])

    def cross(l, m):
        k = l * 3 + m
        return pltpu.make_async_remote_copy(*over(l, m), x_send.at[k], x_recv.at[k], device_id=over_x, device_id_type=MESH)

    def term_down(l, leaving, hook=None):
        side = 1 - chip if leaving else chip
        to = buffers(l, 2, leaving)[0]

        def body(at, right, out_ref):
            out_ref[...] = dot(left_d[...], right[...]).astype(BF16)

        cuts = FB // TN
        if leaving:
            for first, who in ((True, 1 - core), (False, core)):
                block = (side * 2 + who) * cuts
                pipe(body, (cuts,), [pl.BlockSpec((TOKENS, TN), lambda t: (0, block + t))], [pl.BlockSpec((D, TN), lambda t: (0, t))], mids.at[l], to.at[who])
                if first:
                    chip_copy(l, 2, leaving).start()
        else:
            def both(at, right, out_ref):
                if hook:
                    hook(at[0] * cuts + at[1], 2 * cuts)
                body(at, right, out_ref.at[0])

            pipe(both, (2, cuts), [pl.BlockSpec((TOKENS, TN), lambda w, t: (0, (side * 2 + w) * cuts + t))], [pl.BlockSpec((1, D, TN), lambda w, t: (w, 0, t))],
                 mids.at[l], to)
            chip_copy(l, 2, leaving).start()

    def term(l, leaving, ms, hook=None):
        side = 1 - chip if leaving else chip
        to = (out_g if leaving else stay_g).at[l]
        base = ms[0]

        def body(at, right, out_ref):
            if hook:
                hook(at[0] * (FF // TN) + at[1], len(ms) * (FF // TN))
            rows = pl.ds(pl.multiple_of(side * (2 * DB), 128), 2 * DB)
            both = dot(left_a[rows, :], right[0]).astype(BF16)
            out_ref[0, 0] = both[:DB]
            out_ref[0, 1] = both[DB:]

        pipe(body, (len(ms), FF // TN), [pl.BlockSpec((1, TOKENS, TN), lambda m, t: (base + m, 0, t))],
             [pl.BlockSpec((1, 2, DB, TN), lambda m, t: (base + m, 0, 0, t))], dgu.at[l], to)
        for m in ms:
            chip_copy(l, m, leaving).start()

    def leave(l, m):
        named("chip_wait", chip_copy(l, m, 1).wait_recv)
        term, got = buffers(l, m, 1)

        def body(at, mine_ref, got_ref, out_ref):
            out_ref[...] = (mine_ref[...].astype(F32) + got_ref[...].astype(F32)).astype(BF16)

        spec = pl.BlockSpec((D // 4, FB) if m == 2 else (DB // 4, FF), lambda i: (i, 0))
        pipe(body, (4,), [spec, spec], [spec], term.at[core], got, over(l, m)[0])
        cross(l, m).start()

    def by_mid(l):
        rows = 1024

        def body(at, w_ref, silu_ref, slope_ref, dgate_ref, dup_ref):
            for c in range(rows // 256):
                part = slice(c * 256, c * 256 + 256)
                by = dot(dh[pl.ds(at[1] * rows + c * 256, 256), :], w_ref[...], NT).astype(BF16).astype(F32)
                dup_ref[part, :] = (by * silu_ref[part, :]).astype(BF16)
                dgate_ref[part, :] = (by * slope_ref[part, :]).astype(BF16)

        tile = pl.BlockSpec((rows, TN), lambda f, i: (i, f))
        pipe(body, (FF // TN, TOKENS // rows), [pl.BlockSpec((TN, D), lambda f, i: (f, 0)), tile, tile], [tile, tile],
             fd.at[l], silu0, slope0, dgu.at[l, 0], dgu.at[l, 1])

    def by_a(l, meanwhile):
        def scoped(g_w, u_w):
            parts = [(full.at[l, pl.ds(k * 160, 160)], w.at[pl.ds(k * 160, 160)]) for full, w in ((fg, g_w), (fu, u_w)) for k in range(D // 160)]
            copies = [pltpu.make_async_copy(*part, w_sem.at[k]) for k, part in enumerate(parts)]

            def hook(now, steps):
                for step in range(steps):
                    @pl.when(now == step)
                    def _():
                        for c in copies[step * len(copies) // steps:(step + 1) * len(copies) // steps]:
                            c.start()

            meanwhile(hook)
            for c in copies:
                c.wait()

            def body(at, dg_ref, du_ref, h_ref, *out_ref):
                rows = pl.ds(at[0] * 256, 256)
                da = dot(dg_ref[...], g_w[...], NT) + dot(du_ref[...], u_w[...], NT)
                wide = h_ref[...].astype(F32)
                scale = inverse(wide)
                along = jnp.mean(da * wide, -1, keepdims=True)
                new = (dh[rows, :].astype(F32) + scale * (da - wide * (scale * scale * along))).astype(BF16)
                if l:
                    dh[rows, :] = new
                    left_d[:, rows] = new.T
                else:
                    out_ref[0][...] = new

            tile = pl.BlockSpec((256, FF), lambda i: (i, 0))
            named(f"by_a_{l}", pipe, body, (TOKENS // 256,), [tile, tile, row], [] if l else [row], dgu.at[l, 0], dgu.at[l, 1], h1 if l else x, *([] if l else [dx]))

        pl.run_scoped(scoped, pltpu.VMEM((D, FF), BF16), pltpu.VMEM((D, FF), BF16))

    def do(what, *args):
        named("_".join([what.__name__, *[str(v).replace(" ", "") for v in args]]), what, *args)

    named("ready_last", ready, list(range(12, 16)))
    own_copy(1, 2).wait_recv()
    ffn(1, 0, 16, (0, 1, 2, 3))
    ffn(1, 1, 16, (1, 2))
    do(term_down, 1, 1)
    do(leave, 1, 2)
    ffn(1, 2, 16, ())
    ffn(1, 3, 16, ())
    do(term, 1, 1, (0,))
    do(term, 1, 1, (1,))
    do(leave, 1, 0)
    do(leave, 1, 1)
    reload = pltpu.make_async_copy(a0_t, left_a, w_sem.at[16])
    reload.start()
    by_a(1, lambda hook: named("term_down_1_0", term_down, 1, 0, hook))
    do(term_down, 0, 1)
    do(leave, 0, 2)
    do(by_mid, 0)
    reload.wait()
    do(term, 0, 1, (0,))
    do(term, 0, 1, (1,))
    do(leave, 0, 0)
    do(leave, 0, 1)
    do(term, 0, 0, (0, 1))
    reload = pltpu.make_async_copy(a1_t, left_a, w_sem.at[16])
    reload.start()
    do(term_down, 0, 0)
    reload.wait()
    by_a(0, lambda hook: named("term_1_0", term, 1, 0, (0, 1), hook))
    with jax.named_scope("end"):
        for k in range(n):
            for c in (x_copy(k), y_copy(k), first_copy(k), second_copy(k)):
                c.wait_send()
        for l in range(LAYERS):
            for m in range(3):
                own_copy(l, m).wait_send()
                for leaving in (0, 1):
                    chip_copy(l, m, leaving).wait_send()
                chip_copy(l, m, 0).wait_recv()
                cross(l, m).wait()


def total(a, b, c):
    return a.astype(F32) + b.astype(F32) + c.astype(F32)


def finish_kernel(core, stay_g, kept_g, came_g, stay_u, kept_u, came_u, stay_d, kept_d, came_d, dx, og, ou, od, dx_out):
    og[0] = total(stay_g[0, 0, 0], kept_g[0, 0], came_g[0, 0]).astype(BF16)
    ou[0] = total(stay_u[0, 0, 0], kept_u[0, 0], came_u[0, 0]).astype(BF16)
    od[0] = total(stay_d[0, 0], kept_d[0], came_d[0]).astype(BF16).T
    dx_out[...] = dx[...]


def shape(*dims, dtype=BF16):
    return jax.ShapeDtypeStruct(dims, dtype)


def finish(core, stay_g, kept_g, came_g, stay_d, kept_d, came_d, dx):
    steps = 4
    rows, columns, tokens = DB // steps, FB // steps, TOKENS // (LAYERS * steps)
    ins = []
    for m in (0, 1):
        one = pl.BlockSpec((1, 1, rows, FF), lambda l, i, core, m=m: (l, m, i, 0))
        ins += [pl.BlockSpec((1, 1, 1, rows, FF), lambda l, i, core, m=m: (l, m, core[0], i, 0)), one, one]
    one = pl.BlockSpec((1, D, columns), lambda l, i, core: (l, 0, i))
    ins += [pl.BlockSpec((1, 1, D, columns), lambda l, i, core: (l, core[0], 0, i)), one, one]
    some = pl.BlockSpec((tokens, D), lambda l, i, core: (l * steps + i, 0))
    out = pl.BlockSpec((1, rows, FF), lambda l, i, core: (l, i, 0))
    return pl.pallas_call(
        finish_kernel, out_shape=[shape(LAYERS, DB, FF), shape(LAYERS, DB, FF), shape(LAYERS, FB, D), shape(TOKENS, D)],
        compiler_params=pltpu.CompilerParams(vmem_limit_bytes=60 * 2**20),
        grid_spec=pltpu.PrefetchScalarGridSpec(
            num_scalar_prefetch=1, grid=(LAYERS, steps), in_specs=[*ins, some],
            out_specs=[out, out, pl.BlockSpec((1, columns, D), lambda l, i, core: (l, i, 0)), some]),
    )(core, stay_g, kept_g, came_g, stay_g, kept_g, came_g, stay_d, kept_d, came_d, dx)


def body(x, dy, w_gate, w_up, w_down):
    x, dy = x[0], dy[0]
    dma, vmem = pltpu.SemaphoreType.DMA, pltpu.VMEM
    hidden, two_g, one_g, two_d, one_d = shape(LAYERS, TOKENS, FF), shape(LAYERS, 2, 2, DB, FF), shape(LAYERS, 2, DB, FF), shape(LAYERS, 2, D, FB), shape(LAYERS, D, FB)
    outs = dict(
        fg=shape(LAYERS, D, FF), fu=shape(LAYERS, D, FF), fd=shape(LAYERS, FF, D), a0_t=shape(D, TOKENS), a1_t=shape(D, TOKENS),
        silu0=shape(TOKENS, FF, dtype=F32), slope0=shape(TOKENS, FF, dtype=F32), mids=hidden, h1=shape(TOKENS, D), dgu=shape(LAYERS, 2, TOKENS, FF), dx=shape(TOKENS, D),
        out_g=two_g, got_g=one_g, leaves_g=one_g, came_g=one_g, stay_g=two_g, kept_g=one_g,
        out_d=two_d, got_d=one_d, leaves_d=one_d, came_d=one_d, stay_d=two_d, kept_d=one_d)
    n = len(CHUNKS)
    anywhere = pl.BlockSpec(memory_space=pl.ANY)
    done = pl.pallas_call(
        kernel, out_shape=list(outs.values()), in_specs=[anywhere] * 5, out_specs=[anywhere] * len(outs),
        scratch_shapes=[vmem((TOKENS, D), BF16), vmem((TOKENS, D), BF16), vmem((D, TOKENS), BF16), vmem((D, TOKENS), BF16), dma((6,)), dma((6,)), dma((4, n)), dma((4, n)),
                        dma((17,)), dma((12,)), dma((12,)), dma((6,)), dma((6,))],
        compiler_params=pltpu.CompilerParams(collective_id=0, has_side_effects=True, vmem_limit_bytes=60 * 2**20),
        cost_estimate=pl.CostEstimate(flops=17 * 2 * TOKENS * D * FF, bytes_accessed=800_000_000, transcendentals=0),
    )(x, dy, w_gate, w_up, w_down)
    done = dict(zip(outs, done))
    core = (lax.axis_index("dp") % 2).reshape(1).astype(jnp.int32)
    og, ou, od, dx = finish(core, *(done[k] for k in ("stay_g", "kept_g", "came_g", "stay_d", "kept_d", "came_d", "dx")))
    return dx[None], og, ou, od


def solution(mesh):
    own, rows = P(AXES), P(None, "dp")
    return jax.shard_map(body, mesh=mesh, in_specs=(own, own, rows, rows, rows), out_specs=(own, *[P("rep", "dp")] * 3), check_vma=False)
```
